32 devices in a mesh: row: 4 (over x, core), theta: 4 (over z), phi: 2 (over y).
Axes of the slice: x: 2, y: 2, z: 4, core: 2. Of those that a mesh axis runs over, the one named last changes fastest.
Arguments:
- magnetic: float32 [3, 48, 64, 256], P(None, 'row', 'theta', 'phi'), may hold values from -6 to 6
- electric: float32 [3, 48, 64, 256], P(None, 'row', 'theta', 'phi'), may hold values from -6 to 6
Outputs:
- magnetic_new: float32 [3, 48, 64, 256], P(None, 'row', 'theta', 'phi')
- electric_new: float32 [3, 48, 64, 256], P(None, 'row', 'theta', 'phi')
The draws below stay inside these ranges and needn't reach their ends.
All inputs are finite; a program needn't handle non-finite values.
Results may differ from the reference program's by a relative error of at most 0.0001.
Values sent between devices are 32-bit elements; how exact they have to be, the bound alone decides.
A program may use at most 64 MiB of HBM per device.

```python
import math
import jax
import jax.numpy as jnp
from jax import lax

NR = 48
NT = 64
NP = 256


def steps_of(rng, dims, pieces, smallest, high):
    def one(dim, shards_of):
        steps = jax.random.uniform(jax.random.fold_in(jax.random.fold_in(rng, 6), dim), (shards_of,), jnp.float32, smallest / len(pieces), high / len(pieces))
        return jnp.repeat(jnp.exp(steps), dims[dim] // shards_of).reshape((-1,) + (1,) * (len(dims) - dim - 1))

    loudness = one(*pieces[0])
    for cut in pieces[1:]:
        loudness = loudness * one(*cut)
    return loudness


def gaussian(own_key, extent, width, most, shards=(), kind=jnp.bfloat16):
    result = width * jax.random.normal(own_key, extent, jnp.float32)
    if shards:
        result = result * steps_of(own_key, extent, shards, -0.22, 0.18)
    return jnp.clip(result, -most, most).astype(kind)


def setup_inputs(seed: int = 0) -> dict:
    key_of = jax.random.split(jax.random.key(seed), 3)
    return {
        "magnetic": gaussian(key_of[0], (3, NR, NT, NP), 1.0, 6.0, ((1, 4), (2, 4), (3, 2)), jnp.float32),
        "electric": gaussian(key_of[1], (3, NR, NT, NP), 1.0, 6.0, ((1, 4), (2, 4), (3, 2)), jnp.float32),
    }


hole_mass = 1.0
inner_radius = 1.8
wave_speed = 1.25
courant = 0.3
smooth_eps = 1e-06

def weno_face(far_left, near_left, center, near_right, far_right):
    cand_low = (2.0 * far_left - 7.0 * near_left + 11.0 * center) / 6.0
    cand_mid = (-near_left + 5.0 * center + 2.0 * near_right) / 6.0
    cand_high = (2.0 * center + 5.0 * near_right - far_right) / 6.0
    rough_low = 13.0 / 12.0 * (far_left - 2.0 * near_left + center) ** 2 + 0.25 * (far_left - 4.0 * near_left + 3.0 * center) ** 2
    rough_mid = 13.0 / 12.0 * (near_left - 2.0 * center + near_right) ** 2 + 0.25 * (near_left - near_right) ** 2
    rough_high = 13.0 / 12.0 * (center - 2.0 * near_right + far_right) ** 2 + 0.25 * (3.0 * center - 4.0 * near_right + far_right) ** 2
    alpha_low = 0.1 / (smooth_eps + rough_low) ** 2
    alpha_mid = 0.6 / (smooth_eps + rough_mid) ** 2
    alpha_high = 0.3 / (smooth_eps + rough_high) ** 2
    return (alpha_low * cand_low + alpha_mid * cand_mid + alpha_high * cand_high) / (alpha_low + alpha_mid + alpha_high)

def interface(flux, field, axis):
    faces = flux.shape[axis] - 5
    plus_part = 0.5 * (flux + wave_speed * field)
    minus_part = 0.5 * (flux - wave_speed * field)
    plus_cuts = [lax.slice_in_dim(plus_part, offset, offset + faces, axis=axis) for offset in range(6)]
    minus_cuts = [lax.slice_in_dim(minus_part, offset, offset + faces, axis=axis) for offset in range(6)]
    left_state = weno_face(plus_cuts[0], plus_cuts[1], plus_cuts[2], plus_cuts[3], plus_cuts[4])
    right_state = weno_face(minus_cuts[5], minus_cuts[4], minus_cuts[3], minus_cuts[2], minus_cuts[1])
    return left_state + right_state

def face_fluxes(fluxes, fields, axis):
    return lax.map(lambda couple: interface(couple[0], couple[1], axis), (fluxes, fields))

def tendency(padded, radii, angles, spacing_r, spacing_theta, spacing_phi):
    ratio = 2.0 * hole_mass / radii
    lapse_factor = (1.0 / jnp.sqrt(1.0 + ratio))[:, None, None]
    shift_speed = (ratio / (1.0 + ratio))[:, None, None]
    b_radial, b_polar, b_azimuth = (padded[0], padded[1], padded[2])
    d_radial, d_polar, d_azimuth = (padded[3], padded[4], padded[5])
    e_radial = lapse_factor * d_radial
    e_polar = lapse_factor * d_polar - shift_speed * b_azimuth
    e_azimuth = lapse_factor * d_azimuth + shift_speed * b_polar
    h_radial = lapse_factor * b_radial
    h_polar = lapse_factor * b_polar + shift_speed * d_azimuth
    h_azimuth = lapse_factor * b_azimuth - shift_speed * d_polar
    zeros_field = jnp.zeros_like(b_radial)
    radial_flux = jnp.stack([zeros_field, -e_azimuth, e_polar, zeros_field, h_azimuth, -h_polar])
    polar_flux = jnp.stack([e_azimuth, zeros_field, -e_radial, -h_azimuth, zeros_field, h_radial])
    azimuth_flux = jnp.stack([-e_polar, e_radial, zeros_field, h_polar, -h_radial, zeros_field])
    radial_faces = face_fluxes(radial_flux[:, :, 3:-3, 3:-3], padded[:, :, 3:-3, 3:-3], 0)
    polar_faces = face_fluxes(polar_flux[:, 3:-3, :, 3:-3], padded[:, 3:-3, :, 3:-3], 1)
    azimuth_faces = face_fluxes(azimuth_flux[:, 3:-3, 3:-3, :], padded[:, 3:-3, 3:-3, :], 2)
    radius_face = (0.5 * (radii[2:-3] + radii[3:-2])) ** 2
    radius_cell = radii[3:-3] ** 2
    sine_face = jnp.sin(0.5 * (angles[2:-3] + angles[3:-2]))
    sine_cell = jnp.sin(angles[3:-3])
    radial_div = (radius_face[None, 1:, None, None] * radial_faces[:, 1:] - radius_face[None, :-1, None, None] * radial_faces[:, :-1]) / (radius_cell[None, :, None, None] * spacing_r)
    polar_div = (sine_face[None, None, 1:, None] * polar_faces[:, :, 1:] - sine_face[None, None, :-1, None] * polar_faces[:, :, :-1]) / (sine_cell[None, None, :, None] * spacing_theta)
    azimuth_div = (azimuth_faces[:, :, :, 1:] - azimuth_faces[:, :, :, :-1]) / spacing_phi
    return -(radial_div + polar_div + azimuth_div)

def project(fields):
    magnetic_part = fields[:3]
    electric_part = fields[3:]
    b_square = jnp.maximum(lax.optimization_barrier(jnp.sum(magnetic_part * magnetic_part, axis=0)), 1.0)
    along = lax.optimization_barrier(jnp.sum(magnetic_part * electric_part, axis=0)) / b_square
    electric_part = electric_part - along[None] * magnetic_part
    d_square = lax.optimization_barrier(jnp.sum(electric_part * electric_part, axis=0))
    shrink = jnp.sqrt(b_square / jnp.maximum(d_square, b_square))
    return jnp.concatenate([magnetic_part, electric_part * shrink[None]], axis=0)

def extend(fields):
    grown = jnp.pad(fields, ((0, 0), (3, 3), (0, 0), (0, 0)))
    parity = jnp.array([1.0, -1.0, -1.0, 1.0, -1.0, -1.0], jnp.float32)[:, None, None, None]
    half_turn = grown.shape[3] // 2
    north_rows = jnp.roll(grown[:, :, 2::-1, :], half_turn, axis=3) * parity
    south_rows = jnp.roll(grown[:, :, :-4:-1, :], half_turn, axis=3) * parity
    grown = jnp.concatenate([north_rows, grown, south_rows], axis=2)
    return jnp.concatenate([grown[..., -3:], grown, grown[..., :3]], axis=3)

def reference(magnetic, electric):
    fields = jnp.concatenate([magnetic, electric], axis=0)
    spacing_theta = math.pi / NT
    spacing_r = spacing_theta
    spacing_phi = 2.0 * math.pi / NP
    step_dt = courant / (1.0 / spacing_r + 1.0 / spacing_theta + 1.0 / spacing_phi)
    radii = inner_radius + (jnp.arange(-3, NR + 3).astype(jnp.float32) + 0.5) * spacing_r
    angles = (jnp.arange(-3, NT + 3).astype(jnp.float32) + 0.5) * spacing_theta
    current = fields
    for weight in (0.0, 0.75, 1.0 / 3.0):
        rates = tendency(extend(current), radii, angles, spacing_r, spacing_theta, spacing_phi)
        current = project(weight * fields + (1.0 - weight) * (current + step_dt * rates))
    return (current[:3], current[3:])
```

```python
import functools
import math

import jax
import jax.numpy as jnp
from jax import lax
from jax.experimental import pallas as pl
from jax.experimental.pallas import tpu as pltpu
from jax.sharding import PartitionSpec as P

MESH = pl.DeviceIdType.MESH
hole_mass = 1.0
inner_radius = 1.8
wave_speed = 1.25
courant = 0.3
smooth_eps = 1e-06
G = 3
ZERO = ((0, 3), (1, 4), (2, 5))


def flux_of(dim, u, a, s):
    b1, b2, b3, d1, d2, d3 = u
    if dim == 0:
        e2, e3 = a * d2 - s * b3, a * d3 + s * b2
        h2, h3 = a * b2 + s * d3, a * b3 - s * d2
        return [None, -e3, e2, None, h3, -h2]
    if dim == 1:
        e1, e3 = a * d1, a * d3 + s * b2
        h1, h3 = a * b1, a * b3 - s * d2
        return [e3, None, -e1, -h3, None, h1]
    e1, e2 = a * d1, a * d2 - s * b3
    h1, h2 = a * b1, a * b2 + s * d3
    return [-e2, e1, None, h2, -h1, None]


def split(dim, u, a, s):
    out = []
    for f, x in zip(flux_of(dim, u, a, s), u):
        k = wave_speed * x
        out.append((k, -k) if f is None else (f + k, f - k))
    return out


def correction(d0, d1, d2, d3):
    k, eps = 0.609375, 3.0 * smooth_eps
    r1 = (k * d1) * d1 + eps
    r2 = (k * d2) * d2 + eps
    x0 = d0 - 1.375 * d1
    x1 = d1 - 0.625 * d2
    x2 = d3 - 1.375 * d2
    s0, s1, s2 = x0 * x0 + r1, x1 * x1 + r2, x2 * x2 + r2
    s0, s1, s2 = s0 * s0, s1 * s1, s2 * s2
    z = 3.0 * s0
    n0, n2, y = s1 * s2, z * s1, z * s2
    den = (n0 + n2) + (y + y)
    t2 = d2 - d1
    t_low = t2 - (d1 - d0)
    t_high = (d3 - d2) - t2
    return ((n0 + n0) * t_low + n2 * t_high) * pl.reciprocal(den, approx=True)


def face(p, m):
    dp = [p[i + 1] - p[i] for i in range(4)]
    dm = [m[i + 1] - m[i] for i in range(4)]
    cp = correction(dp[0], dp[1], dp[2], dp[3])
    cm = correction(dm[3], dm[2], dm[1], dm[0])
    lin = 5.0 * (p[2] + m[2]) + 2.0 * (p[3] + m[1]) - (p[1] + m[3])
    return lin - (cp - cm)


def kernel(sizes, mag, ele, mag_out, ele_out, u, pa, pb, ra, rb, te, tr, fr, acc, vr, vt, gb, pd,
           ca, cs, crp, crm, cth, send, recv, local):
    n_row, n_theta, n_phi, nr, nt, L, plane = sizes
    row, th, ph = lax.axis_index("row"), lax.axis_index("theta"), lax.axis_index("phi")
    slot = L // nr
    halves = nt // 8
    spacing = math.pi / (nt * n_theta)
    spacing_phi = 2.0 * math.pi / (L * n_phi)
    dt = courant / (1.0 / spacing + 1.0 / spacing + 1.0 / spacing_phi)
    scale = -dt / 12.0
    planes = nr + 2 * G
    flat = u.reshape(u.shape[0], 6, (planes + 2) * plane, L)
    first, last = th == 0, th == n_theta - 1
    opposite = (row, th, lax.rem(ph + n_phi // 2, n_phi))
    right = (row, th, lax.rem(ph + 1, n_phi))
    left = (row, th, lax.rem(ph + n_phi - 1, n_phi))
    above = tuple(jnp.where(last, o, q) for o, q in zip(opposite, (row, th + 1, ph)))
    below = tuple(jnp.where(first, o, q) for o, q in zip(opposite, (row, th - 1, ph)))
    outer, inner = (row + 1, th, ph), (row - 1, th, ph)
    has_outer, has_inner = row < n_row - 1, row > 0

    loads = [
        pltpu.make_async_copy(src, u.at[0, 3 * i : 3 * i + 3, 1 + G : 1 + G + nr, 0:nt], local.at[i])
        for i, src in enumerate((mag, ele))
    ]
    for c in loads:
        c.start()

    barrier = pltpu.get_barrier_semaphore()
    for target in (above, below, right, left):
        pl.semaphore_signal(barrier, inc=1, device_id=target, device_id_type=MESH)

    @pl.when(has_outer)
    def _():
        pl.semaphore_signal(barrier, inc=1, device_id=outer, device_id_type=MESH)

    @pl.when(has_inner)
    def _():
        pl.semaphore_signal(barrier, inc=1, device_id=inner, device_id_type=MESH)

    lane = lax.broadcasted_iota(jnp.int32, (8, L), 1)
    sub = lax.broadcasted_iota(jnp.int32, (8, L), 0)
    owner = jnp.zeros((8, L), jnp.int32)
    for q in range(1, nr):
        owner = owner + (lane >= slot * q).astype(jnp.int32)
    in_slot = lane - slot * owner

    def radius_at(index):
        return inner_radius + (index.astype(jnp.float32) + 0.5) * spacing

    def lapse_shift(radius):
        ratio = 2.0 * hole_mass / radius
        return 1.0 / jnp.sqrt(1.0 + ratio), ratio / (1.0 + ratio)

    for q in range(ca.shape[0] // 8):
        a, s = lapse_shift(radius_at(row * nr - G + 8 * q + sub))
        ca[8 * q : 8 * q + 8] = a
        cs[8 * q : 8 * q + 8] = s
    for q in range(crp.shape[0] // 8):
        index = row * nr + 8 * q + sub
        rc, hi, lo = radius_at(index), radius_at(index + 1), radius_at(index - 1)
        crp[8 * q : 8 * q + 8] = scale * (0.5 * (rc + hi)) ** 2 / (rc * rc * spacing)
        crm[8 * q : 8 * q + 8] = scale * (0.5 * (rc + lo)) ** 2 / (rc * rc * spacing)
    for q in range(halves):
        index = (th * nt + 8 * q + sub).astype(jnp.float32)
        mid = jnp.sin((index + 0.5) * spacing)
        cth[0, 8 * q : 8 * q + 8] = scale * jnp.sin((index + 1.0) * spacing) / (mid * spacing)
        cth[1, 8 * q : 8 * q + 8] = scale * jnp.sin(index * spacing) / (mid * spacing)
    a_lane, s_lane = lapse_shift(radius_at(row * nr + owner))
    coef_phi = scale / spacing_phi

    zeros = jnp.zeros((nt, L), jnp.float32)
    for stage in range(3):
        @pl.when(row == 0)
        def _():
            for c in range(6):
                for q in range(G):
                    u[stage, c, 1 + q, 0:nt] = zeros

        @pl.when(row == n_row - 1)
        def _():
            for c in range(6):
                for q in range(G):
                    u[stage, c, 1 + G + nr + q, 0:nt] = zeros

    def pack(stage, r, tiles):
        mask = (lane >= slot * r) & (lane < slot * r + slot)
        for c in range(6):
            for t in range(halves):
                x = tiles[c][t]
                pa[stage, c, t] = jnp.where(mask, pltpu.roll(x, slot * r + 3, 1), pa[stage, c, t])
                pb[stage, c, t] = jnp.where(
                    mask, pltpu.roll(x, lax.rem(slot * r + 6, L), 1), pb[stage, c, t]
                )

    def tile(stage, c, r, t):
        return u[stage, c, 1 + G + r, 8 * t : 8 * t + 8]

    def remote(src, dst, stage, m_send, m_recv, target):
        return pltpu.make_async_remote_copy(
            src_ref=src, dst_ref=dst, send_sem=send.at[stage, m_send], recv_sem=recv.at[stage, m_recv],
            device_id=target, device_id_type=MESH,
        )

    base = 1 + G

    def radial_out(stage):
        return remote(u.at[stage, :, base + nr - G : base + nr, 0:nt], u.at[stage, :, 1 : 1 + G, 0:nt],
                      stage, 0, 0, outer)

    def radial_in(stage):
        return remote(u.at[stage, :, base : base + G, 0:nt],
                      u.at[stage, :, base + nr : base + nr + G, 0:nt], stage, 1, 1, inner)

    def theta_copies(stage):
        up = jnp.where(last, 1, 0)
        down = jnp.where(first, 0, 1)
        return (
            remote(te.at[stage, 1], tr.at[stage, up], stage, 2, 2 + up, above),
            remote(te.at[stage, 0], tr.at[stage, down], stage, 3, 2 + down, below),
        )

    def phi_copies(stage):
        return (
            remote(pa.at[stage], ra.at[stage], stage, 4, 4, right),
            remote(pb.at[stage], rb.at[stage], stage, 5, 5, left),
        )

    starts = list(range(0, nr - 7, 8))
    if starts[-1] + 8 < nr:
        starts.append(nr - 8)

    def grab(stage, c, r0, k):
        return flat[stage, c, pl.ds((base + r0) * plane + k, 8, stride=plane), :]

    def send_all(stage):
        @pl.when(has_outer)
        def _():
            radial_out(stage).start()

        @pl.when(has_inner)
        def _():
            radial_in(stage).start()

        for side in range(2):
            for c in range(6):
                for k in range(G):
                    for r0 in starts:
                        te[stage, side, pl.ds((c * G + k) * nr + r0, 8), :] = grab(
                            stage, c, r0, k if side == 0 else nt - G + k
                        )
        for c in theta_copies(stage) + phi_copies(stage):
            c.start()

    for c in loads:
        c.wait()

    def pack_first(r, carry):
        pack(0, r, [[tile(0, c, r, t) for t in range(halves)] for c in range(6)])
        return carry

    lax.fori_loop(0, nr, pack_first, 0)
    pl.semaphore_wait(barrier, 4 + jnp.where(has_outer, 1, 0) + jnp.where(has_inner, 1, 0))
    send_all(0)

    def rolled(v, k):
        return v if k == 0 else pltpu.roll(v, (-k) % L, 1)

    def phi_div(split_values):
        out = []
        for c, (vp, vm) in enumerate(split_values):
            p = [rolled(vp, k) for k in range(-2, 3)]
            if c in ZERO[2]:
                m = [-x for x in p[1:]] + [rolled(vm, 3)]
            else:
                m = [rolled(vm, k) for k in range(-1, 4)]
            f = face(p, m)
            out.append(coef_phi * (f - pltpu.roll(f, 1, 1)))
        return out

    def coefs(p):
        return (
            jnp.broadcast_to(ca[pl.ds(p, 1), :], (8, L)),
            jnp.broadcast_to(cs[pl.ds(p, 1), :], (8, L)),
        )

    def stage_body(stage, carry):
        def phi_pass(r, carry):
            a, s = coefs(r + G)
            for t in range(halves):
                x = [tile(stage, c, r, t) for c in range(6)]
                for c, d in enumerate(phi_div(split(2, x, a, s))):
                    acc[c, r, 8 * t : 8 * t + 8] = d
                for c, (vp, vm) in enumerate(split(0, x, a, s)):
                    vr[0, c, r + G, 8 * t : 8 * t + 8] = vp
                    vr[1, c, r + G, 8 * t : 8 * t + 8] = vm
            return carry

        lax.fori_loop(0, nr, phi_pass, 0)

        def radial_face(f, carry):
            for c in range(6):
                for t in range(halves):
                    rows = slice(8 * t, 8 * t + 8)
                    p = [vr[0, c, f + k, rows] for k in range(5)]
                    m = [vr[1, c, f + k, rows] for k in range(1, 6)]
                    fr[c, f, rows] = face(p, m)
            return carry

        lax.fori_loop(G, nr - G + 1, radial_face, 0)

        @pl.when(has_inner)
        def _():
            radial_out(stage).wait_recv()

        @pl.when(has_outer)
        def _():
            radial_in(stage).wait_recv()

        def ghost_planes(q, carry):
            p = jnp.where(q < G, q, q + nr)
            a, s = coefs(p)
            for t in range(halves):
                x = [u[stage, c, 1 + p, 8 * t : 8 * t + 8] for c in range(6)]
                for c, (vp, vm) in enumerate(split(0, x, a, s)):
                    vr[0, c, p, 8 * t : 8 * t + 8] = vp
                    vr[1, c, p, 8 * t : 8 * t + 8] = vm
            return carry

        lax.fori_loop(0, 2 * G, ghost_planes, 0)

        def outer_faces(q, carry):
            return radial_face(jnp.where(q < G, q, q + nr + 1 - 2 * G), carry)

        lax.fori_loop(0, 2 * G, outer_faces, 0)

        for side in range(2):
            remote(te.at[stage, side], tr.at[stage, side], stage, 2, 2 + side, above).wait_recv()
            pole = first if side == 0 else last
            sign = jnp.where(pole, -1.0, 1.0)
            for g in range(G):
                k = jnp.where(pole, G - 1 - g, g)
                for c in range(6):
                    for r0 in starts:
                        x = tr[stage, side, pl.ds((c * G + k) * nr + r0, 8), :]
                        if c % 3:
                            x = x * sign
                        target = (base + r0) * plane + (g - G if side == 0 else nt + g)
                        flat[stage, c, pl.ds(target, 8, stride=plane), :] = x

        for r0 in starts:
            a, s = ca[G + r0 : G + r0 + 8], cs[G + r0 : G + r0 + 8]
            v = [split(1, [grab(stage, c, r0, k) for c in range(6)], a, s) for k in range(-3, 3)]
            for c in range(6):
                gb[c, r0 : r0 + 8] = face([v[k][c][0] for k in range(5)], [v[k][c][1] for k in range(1, 6)])

        for c in phi_copies(stage):
            c.wait_recv()

        def packed(t, carry):
            xa = [jnp.where(in_slot < 3, ra[stage, c, t], pa[stage, c, t]) for c in range(6)]
            xb = [jnp.where(in_slot >= 6, rb[stage, c, t], pb[stage, c, t]) for c in range(6)]
            da = phi_div(split(2, xa, a_lane, s_lane))
            db = phi_div(split(2, xb, a_lane, s_lane))
            for c in range(6):
                pd[c, t] = jnp.where(in_slot < 6, db[c], pltpu.roll(da[c], 3, 1))
            return carry

        lax.fori_loop(0, halves, packed, 0)

        w = jnp.where(stage == 0, 0.0, jnp.where(stage == 1, 0.75, 1.0 / 3.0)).astype(jnp.float32)
        edge = (lane < 3) | (lane >= L - 3)

        def final(r, carry):
            a, s = coefs(r + G)
            top = (base + r) * plane - G
            for q in range(halves + 1):
                x = [flat[stage, c, pl.ds(top + 8 * q, 8), :] for c in range(6)]
                for c, (vp, vm) in enumerate(split(1, x, a, s)):
                    vt[0, c, 8 * q : 8 * q + 8] = vp
                    vt[1, c, 8 * q : 8 * q + 8] = vm
            rp = jnp.broadcast_to(crp[pl.ds(r, 1), :], (8, L))
            rm = jnp.broadcast_to(crm[pl.ds(r, 1), :], (8, L))
            new = [[None] * halves for _ in range(6)]
            for c in range(6):
                before = jnp.broadcast_to(gb[c, pl.ds(r, 1), :], (8, L))
                for t in range(halves):
                    rows = slice(8 * t, 8 * t + 8)
                    f = face([vt[0, c, 8 * t + k : 8 * t + k + 8] for k in range(1, 6)],
                             [vt[1, c, 8 * t + k : 8 * t + k + 8] for k in range(2, 7)])
                    turned = pltpu.roll(f, 1, 0)
                    lower = jnp.where(sub == 0, before, turned)
                    before = turned
                    patch = pltpu.roll(pd[c, t], lax.rem(L + L - 6 - slot * r, L), 1)
                    rate = jnp.where(edge, patch, acc[c, r, rows])
                    rate = rate + (cth[0, rows] * f - cth[1, rows] * lower)
                    rate = rate + (rp * fr[c, r + 1, rows] - rm * fr[c, r, rows])
                    new[c][t] = w * tile(0, c, r, t) + (1.0 - w) * (tile(stage, c, r, t) + rate)
            for t in range(halves):
                b, d = [new[c][t] for c in range(3)], [new[c][t] for c in range(3, 6)]
                b2 = jnp.maximum(b[0] * b[0] + b[1] * b[1] + b[2] * b[2], 1.0)
                along = (b[0] * d[0] + b[1] * d[1] + b[2] * d[2]) / b2
                d = [y - along * x for x, y in zip(b, d)]
                d2 = d[0] * d[0] + d[1] * d[1] + d[2] * d[2]
                shrink = jnp.sqrt(b2 / jnp.maximum(d2, b2))
                for c in range(3):
                    new[3 + c][t] = d[c] * shrink
                for c in range(6):
                    u[stage + 1, c, base + r, 8 * t : 8 * t + 8] = new[c][t]

            @pl.when(stage < 2)
            def _():
                pack(stage + 1, r, new)

            return carry

        lax.fori_loop(0, nr, final, 0)

        @pl.when(stage < 2)
        def _():
            send_all(stage + 1)

        return carry

    lax.fori_loop(0, 3, stage_body, 0)
    stores = [
        pltpu.make_async_copy(u.at[3, 3 * i : 3 * i + 3, base : base + nr, 0:nt], dst, local.at[i])
        for i, dst in enumerate((mag_out, ele_out))
    ]
    for c in stores:
        c.start()

    def drain(stage, carry):
        @pl.when(has_outer)
        def _():
            radial_out(stage).wait_send()

        @pl.when(has_inner)
        def _():
            radial_in(stage).wait_send()

        for c in theta_copies(stage) + phi_copies(stage):
            c.wait_send()
        return carry

    lax.fori_loop(0, 3, drain, 0)
    for c in stores:
        c.wait()


def solution(mesh):
    n_row, n_theta, n_phi = (mesh.shape[k] for k in ("row", "theta", "phi"))

    def body(magnetic, electric):
        _, nr, nt, lanes = magnetic.shape
        plane = -(-(nt + 2 * G) // 8) * 8
        planes = nr + 2 * G
        halves = nt // 8
        pad8 = lambda n: -(-n // 8) * 8
        f32 = jnp.float32
        vm = lambda *shape: pltpu.VMEM(shape, f32)
        sizes = (n_row, n_theta, n_phi, nr, nt, lanes, plane)
        anywhere = pl.BlockSpec(memory_space=pl.ANY)
        packs = vm(3, 6, halves, 8, lanes)
        return pl.pallas_call(
            functools.partial(kernel, sizes),
            out_shape=[jax.ShapeDtypeStruct(magnetic.shape, f32)] * 2,
            in_specs=[anywhere] * 2,
            out_specs=[anywhere] * 2,
            scratch_shapes=[
                vm(4, 6, planes + 2, plane, lanes),
                packs, packs, packs, packs,
                vm(3, 2, 6 * G * nr, lanes),
                vm(3, 2, 6 * G * nr, lanes),
                vm(6, nr + 1, nt, lanes),
                vm(6, nr, nt, lanes),
                vm(2, 6, planes, nt, lanes),
                vm(2, 6, nt + 8, lanes),
                vm(6, pad8(nr), lanes),
                vm(6, halves, 8, lanes),
                vm(pad8(planes), lanes),
                vm(pad8(planes), lanes),
                vm(pad8(nr), lanes),
                vm(pad8(nr), lanes),
                vm(2, nt, lanes),
                pltpu.SemaphoreType.DMA((3, 6)),
                pltpu.SemaphoreType.DMA((3, 6)),
                pltpu.SemaphoreType.DMA((2,)),
            ],
            compiler_params=pltpu.CompilerParams(collective_id=0, has_side_effects=True),
        )(magnetic, electric)

    spec = P(None, "row", "theta", "phi")
    return jax.shard_map(body, mesh=mesh, in_specs=(spec, spec), out_specs=(spec, spec), check_vma=False)
```

```python
import functools
import math

import jax
import jax.numpy as jnp
from jax import lax
from jax.experimental import pallas as pl
from jax.experimental.pallas import tpu as pltpu
from jax.sharding import PartitionSpec as P

MESH = pl.DeviceIdType.MESH
hole_mass = 1.0
inner_radius = 1.8
wave_speed = 1.25
courant = 0.3
smooth_eps = 1e-06
G = 3
ZERO = ((0, 3), (1, 4), (2, 5))


def flux_of(dim, u, a, s):
    b1, b2, b3, d1, d2, d3 = u
    if dim == 0:
        e2, e3 = a * d2 - s * b3, a * d3 + s * b2
        h2, h3 = a * b2 + s * d3, a * b3 - s * d2
        return [None, -e3, e2, None, h3, -h2]
    if dim == 1:
        e1, e3 = a * d1, a * d3 + s * b2
        h1, h3 = a * b1, a * b3 - s * d2
        return [e3, None, -e1, -h3, None, h1]
    e1, e2 = a * d1, a * d2 - s * b3
    h1, h2 = a * b1, a * b2 + s * d3
    return [-e2, e1, None, h2, -h1, None]


def split(dim, u, a, s):
    out = []
    for f, x in zip(flux_of(dim, u, a, s), u):
        k = wave_speed * x
        out.append((k, -k) if f is None else (f + k, f - k))
    return out


class Line:
    def __init__(self, d, r=None, t3=None):
        self.made, self.d0, self.r0, self.t0 = {}, d, r, t3

    def keep(self, kind, i, make):
        if (kind, i) not in self.made:
            self.made[kind, i] = make()
        return self.made[kind, i]

    def d(self, i):
        return self.keep(0, i, lambda: self.d0(i))

    def square(self, i):
        k, eps = 0.609375, 3.0 * smooth_eps
        return (k * self.d(i)) * self.d(i) + eps

    def r(self, i):
        return self.keep(1, i, lambda: self.r0(i) if self.r0 else self.square(i))

    def q(self, i):
        return self.keep(2, i, lambda: 1.375 * self.d(i))

    def h(self, i):
        return self.keep(3, i, lambda: 0.625 * self.d(i))

    def step(self, i):
        return self.keep(4, i, lambda: self.d(i) - self.d(i - 1))

    def third(self, i):
        return self.step(i + 1) - self.step(i)

    def t(self, i):
        return self.keep(5, i, lambda: self.t0(i) if self.t0 else self.third(i))


def correction(line, i, way):
    i0, i1, i3 = i - 2 * way, i - way, i + way
    x0 = line.d(i0) - line.q(i1)
    x1 = line.d(i1) - line.h(i)
    x2 = line.d(i3) - line.q(i)
    s0, s1, s2 = x0 * x0 + line.r(i1), x1 * x1 + line.r(i), x2 * x2 + line.r(i)
    s0, s1, s2 = s0 * s0, s1 * s1, s2 * s2
    z = 3.0 * s0
    n0, n2, y = s1 * s2, z * s1, z * s2
    den = (n0 + n2) + (y + y)
    return ((n0 + n0) * line.t(i1) + n2 * line.t(i)) * pl.reciprocal(den, approx=True)


def face(p, m, double, i=0):
    if m is None:
        return p.t(i) - (correction(p, i, 1) + correction(p, i, -1))
    dm = m.d(i)
    lin = 6.0 * double + ((p.d(i - 1) - m.d(i + 1)) + 2.0 * (p.d(i) + (dm + dm)))
    return lin - (correction(p, i, 1) - correction(m, i, -1))


def line_of(values, start=0):
    return Line(lambda i: values[i + 1 - start] - values[i - start])


def kernel(sizes, mag, ele, mag_out, ele_out, u, pa, pb, sa, sb, ra, rb, te, tr, fr, acc, vr, vt, vd, vs, gb, pd,
           ca, cs, crp, crm, cth, send, recv, local):
    n_row, n_theta, n_phi, nr, nt, L, plane = sizes
    row, th, ph = lax.axis_index("row"), lax.axis_index("theta"), lax.axis_index("phi")
    slot = L // nr
    halves = nt // 8
    spacing = math.pi / (nt * n_theta)
    spacing_phi = 2.0 * math.pi / (L * n_phi)
    dt = courant / (1.0 / spacing + 1.0 / spacing + 1.0 / spacing_phi)
    scale = -dt / 12.0
    planes = nr + 2 * G
    flat = u.reshape(u.shape[0], 6, (planes + 2) * plane, L)
    first, last = th == 0, th == n_theta - 1
    opposite = (row, th, lax.rem(ph + n_phi // 2, n_phi))
    right = (row, th, lax.rem(ph + 1, n_phi))
    left = (row, th, lax.rem(ph + n_phi - 1, n_phi))
    above = tuple(jnp.where(last, o, q) for o, q in zip(opposite, (row, th + 1, ph)))
    below = tuple(jnp.where(first, o, q) for o, q in zip(opposite, (row, th - 1, ph)))
    outer, inner = (row + 1, th, ph), (row - 1, th, ph)
    has_outer, has_inner = row < n_row - 1, row > 0

    loads = [
        pltpu.make_async_copy(src, u.at[0, 3 * i : 3 * i + 3, 1 + G : 1 + G + nr, 0:nt], local.at[i])
        for i, src in enumerate((mag, ele))
    ]
    for c in loads:
        c.start()

    barrier = pltpu.get_barrier_semaphore()
    for target in (above, below, right, left):
        pl.semaphore_signal(barrier, inc=1, device_id=target, device_id_type=MESH)

    @pl.when(has_outer)
    def _():
        pl.semaphore_signal(barrier, inc=1, device_id=outer, device_id_type=MESH)

    @pl.when(has_inner)
    def _():
        pl.semaphore_signal(barrier, inc=1, device_id=inner, device_id_type=MESH)

    lane = lax.broadcasted_iota(jnp.int32, (8, L), 1)
    sub = lax.broadcasted_iota(jnp.int32, (8, L), 0)
    owner = jnp.zeros((8, L), jnp.int32)
    for q in range(1, nr):
        owner = owner + (lane >= slot * q).astype(jnp.int32)
    in_slot = lane - slot * owner

    def radius_at(index):
        return inner_radius + (index.astype(jnp.float32) + 0.5) * spacing

    def lapse_shift(radius):
        ratio = 2.0 * hole_mass / radius
        return 1.0 / jnp.sqrt(1.0 + ratio), ratio / (1.0 + ratio)

    for q in range(ca.shape[0] // 8):
        a, s = lapse_shift(radius_at(row * nr - G + 8 * q + sub))
        ca[8 * q : 8 * q + 8] = a
        cs[8 * q : 8 * q + 8] = s
    for q in range(crp.shape[0] // 8):
        index = row * nr + 8 * q + sub
        rc, hi, lo = radius_at(index), radius_at(index + 1), radius_at(index - 1)
        crp[8 * q : 8 * q + 8] = scale * (0.5 * (rc + hi)) ** 2 / (rc * rc * spacing)
        crm[8 * q : 8 * q + 8] = scale * (0.5 * (rc + lo)) ** 2 / (rc * rc * spacing)
    for q in range(halves):
        index = (th * nt + 8 * q + sub).astype(jnp.float32)
        mid = jnp.sin((index + 0.5) * spacing)
        cth[0, 8 * q : 8 * q + 8] = scale * jnp.sin((index + 1.0) * spacing) / (mid * spacing)
        cth[1, 8 * q : 8 * q + 8] = scale * jnp.sin(index * spacing) / (mid * spacing)
    a_lane, s_lane = lapse_shift(radius_at(row * nr + owner))
    coef_phi = scale / spacing_phi

    zeros = jnp.zeros((nt, L), jnp.float32)
    for stage in range(3):
        @pl.when(row == 0)
        def _():
            for c in range(6):
                for q in range(G):
                    u[stage, c, 1 + q, 0:nt] = zeros

        @pl.when(row == n_row - 1)
        def _():
            for c in range(6):
                for q in range(G):
                    u[stage, c, 1 + G + nr + q, 0:nt] = zeros

    def pack(stage, r, tiles):
        mask = (lane >= slot * r) & (lane < slot * r + slot)
        for c in range(6):
            for t in range(halves):
                x = tiles[c][t]
                pa[stage, c, t] = jnp.where(mask, pltpu.roll(x, slot * r + 3, 1), pa[stage, c, t])
                pb[stage, c, t] = jnp.where(
                    mask, pltpu.roll(x, lax.rem(slot * r + 6, L), 1), pb[stage, c, t]
                )

    def tile(stage, c, r, t):
        return u[stage, c, 1 + G + r, 8 * t : 8 * t + 8]

    def remote(src, dst, stage, m_send, m_recv, target):
        return pltpu.make_async_remote_copy(
            src_ref=src, dst_ref=dst, send_sem=send.at[stage, m_send], recv_sem=recv.at[stage, m_recv],
            device_id=target, device_id_type=MESH,
        )

    base = 1 + G

    def radial_out(stage):
        return remote(u.at[stage, :, base + nr - G : base + nr, 0:nt], u.at[stage, :, 1 : 1 + G, 0:nt],
                      stage, 0, 0, outer)

    def radial_in(stage):
        return remote(u.at[stage, :, base : base + G, 0:nt],
                      u.at[stage, :, base + nr : base + nr + G, 0:nt], stage, 1, 1, inner)

    def theta_copies(stage):
        up = jnp.where(last, 1, 0)
        down = jnp.where(first, 0, 1)
        return (
            remote(te.at[stage, 1], tr.at[stage, up], stage, 2, 2 + up, above),
            remote(te.at[stage, 0], tr.at[stage, down], stage, 3, 2 + down, below),
        )

    def phi_copies(stage):
        return (
            remote(sa.at[stage], ra.at[stage], stage, 4, 4, right),
            remote(sb.at[stage], rb.at[stage], stage, 5, 5, left),
        )

    starts = list(range(0, nr - 7, 8))
    if starts[-1] + 8 < nr:
        starts.append(nr - 8)

    def grab(stage, c, r0, k):
        return flat[stage, c, pl.ds((base + r0) * plane + k, 8, stride=plane), :]

    def send_all(stage):
        @pl.when(has_outer)
        def _():
            radial_out(stage).start()

        @pl.when(has_inner)
        def _():
            radial_in(stage).start()

        for g in range(2):
            for t in range(halves):
                x, y = pa[stage, 3 * g + 1, t], pa[stage, 3 * g + 2, t]
                x = jnp.where(in_slot < 6, pltpu.roll(x, 3, 1), pltpu.roll(y, 6, 1))
                sa[stage, g, t] = jnp.where(in_slot < 3, pa[stage, 3 * g, t], x)
                x, y = pb[stage, 3 * g + 1, t], pb[stage, 3 * g + 2, t]
                x = jnp.where(in_slot < 3, pltpu.roll(y, L - 6, 1), pltpu.roll(x, L - 3, 1))
                sb[stage, g, t] = jnp.where(in_slot < 6, x, pb[stage, 3 * g, t])
        for side in range(2):
            for c in range(6):
                for k in range(G):
                    for r0 in starts:
                        te[stage, side, pl.ds((c * G + k) * nr + r0, 8), :] = grab(
                            stage, c, r0, k if side == 0 else nt - G + k
                        )
        for c in theta_copies(stage) + phi_copies(stage):
            c.start()

    for c in loads:
        c.wait()

    def pack_first(r, carry):
        pack(0, r, [[tile(0, c, r, t) for t in range(halves)] for c in range(6)])
        return carry

    lax.fori_loop(0, nr, pack_first, 0)
    pl.semaphore_wait(barrier, 4 + jnp.where(has_outer, 1, 0) + jnp.where(has_inner, 1, 0))
    send_all(0)

    def rolled(v, k):
        return v if k == 0 else pltpu.roll(v, (-k) % L, 1)

    def turning(v):
        made = {}

        def at(kind, i, make):
            if i == 0:
                if kind not in made:
                    made[kind] = make()
                return made[kind]
            return rolled(at(kind, 0, make), i)

        line = Line(
            lambda i: at(0, i, lambda: rolled(v, 1) - v),
            lambda i: at(1, i, lambda: line.square(0)),
            lambda i: at(2, i, lambda: line.third(0)),
        )
        return line

    def phi_div(split_values):
        out = []
        for c, (vp, vm) in enumerate(split_values):
            f = face(turning(vp), None if c in ZERO[2] else turning(vm), vp + vm)
            out.append(coef_phi * (f - pltpu.roll(f, 1, 1)))
        return out

    def coefs(p):
        return (
            jnp.broadcast_to(ca[pl.ds(p, 1), :], (8, L)),
            jnp.broadcast_to(cs[pl.ds(p, 1), :], (8, L)),
        )

    def stage_body(stage, carry):
        def phi_pass(r, carry):
            a, s = coefs(r + G)
            for t in range(halves):
                x = [tile(stage, c, r, t) for c in range(6)]
                for c, d in enumerate(phi_div(split(2, x, a, s))):
                    acc[c, r, 8 * t : 8 * t + 8] = d
                for c, (vp, vm) in enumerate(split(0, x, a, s)):
                    vr[0, c, r + G, 8 * t : 8 * t + 8] = vp
                    vr[1, c, r + G, 8 * t : 8 * t + 8] = vm
            return carry

        lax.fori_loop(0, nr, phi_pass, 0)

        def radial_faces(lo, hi):
            def part(t, carry):
                rows = pl.ds(pl.multiple_of(8 * t, 8), 8)
                for c in range(6):
                    p = [vr[0, c, k, rows] for k in range(lo, hi + 5)]
                    pline, mline, m = line_of(p, lo), None, None
                    if c not in ZERO[0]:
                        m = [vr[1, c, k, rows] for k in range(lo, hi + 5)]
                        mline = line_of(m, lo)
                    for f in range(lo, hi):
                        i = f + 2
                        double = None if m is None else p[i - lo] + m[i - lo]
                        fr[c, f, rows] = face(pline, mline, double, i)
                return carry

            lax.fori_loop(0, halves, part, 0)

        radial_faces(G, nr - G + 1)

        @pl.when(has_inner)
        def _():
            radial_out(stage).wait_recv()

        @pl.when(has_outer)
        def _():
            radial_in(stage).wait_recv()

        def ghost_planes(q, carry):
            p = jnp.where(q < G, q, q + nr)
            a, s = coefs(p)
            for t in range(halves):
                x = [u[stage, c, 1 + p, 8 * t : 8 * t + 8] for c in range(6)]
                for c, (vp, vm) in enumerate(split(0, x, a, s)):
                    vr[0, c, p, 8 * t : 8 * t + 8] = vp
                    vr[1, c, p, 8 * t : 8 * t + 8] = vm
            return carry

        lax.fori_loop(0, 2 * G, ghost_planes, 0)

        radial_faces(0, G)
        radial_faces(nr - G + 1, nr + 1)

        for side in range(2):
            remote(te.at[stage, side], tr.at[stage, side], stage, 2, 2 + side, above).wait_recv()
            pole = first if side == 0 else last
            sign = jnp.where(pole, -1.0, 1.0)
            for g in range(G):
                k = jnp.where(pole, G - 1 - g, g)
                for c in range(6):
                    for r0 in starts:
                        x = tr[stage, side, pl.ds((c * G + k) * nr + r0, 8), :]
                        if c % 3:
                            x = x * sign
                        target = (base + r0) * plane + (g - G if side == 0 else nt + g)
                        flat[stage, c, pl.ds(target, 8, stride=plane), :] = x

        for r0 in starts:
            a, s = ca[G + r0 : G + r0 + 8], cs[G + r0 : G + r0 + 8]
            v = [split(1, [grab(stage, c, r0, k) for c in range(6)], a, s) for k in range(-3, 3)]
            for c in range(6):
                pline = line_of([v[k][c][0] for k in range(6)], -2)
                mline = None if c in ZERO[1] else line_of([v[k][c][1] for k in range(6)], -2)
                gb[c, r0 : r0 + 8] = face(pline, mline, v[2][c][0] + v[2][c][1])

        for c in phi_copies(stage):
            c.wait_recv()

        def packed(t, carry):
            xa = [
                jnp.where(in_slot < 3, rolled(ra[stage, c // 3, t], 3 * (c % 3)), pa[stage, c, t])
                for c in range(6)
            ]
            xb = [
                jnp.where(in_slot >= 6, rolled(rb[stage, c // 3, t], -3 * (c % 3)), pb[stage, c, t])
                for c in range(6)
            ]
            da = phi_div(split(2, xa, a_lane, s_lane))
            db = phi_div(split(2, xb, a_lane, s_lane))
            for c in range(6):
                pd[c, t] = jnp.where(in_slot < 6, db[c], pltpu.roll(da[c], 3, 1))
            return carry

        lax.fori_loop(0, halves, packed, 0)

        w = jnp.where(stage == 0, 0.0, jnp.where(stage == 1, 0.75, 1.0 / 3.0)).astype(jnp.float32)
        edge = (lane < 3) | (lane >= L - 3)

        def final(r, carry):
            a, s = coefs(r + G)
            top = (base + r) * plane - G
            for q in range(halves + 1):
                x = [flat[stage, c, pl.ds(top + 8 * q, 8), :] for c in range(6)]
                for c, values in enumerate(split(1, x, a, s)):
                    for sign, v in enumerate(values):
                        vt[sign, c, 8 * q : 8 * q + 8] = v
            for c in range(6):
                for sign in range(1 if c in ZERO[1] else 2):
                    for q in range(halves + 1):
                        d = vt[sign, c, 8 * q + 1 : 8 * q + 9] - vt[sign, c, 8 * q : 8 * q + 8]
                        vd[sign, c, 8 * q : 8 * q + 8] = d
                        vs[sign, c, 8 * q : 8 * q + 8] = Line(lambda i: d).square(0)
            rp = jnp.broadcast_to(crp[pl.ds(r, 1), :], (8, L))
            rm = jnp.broadcast_to(crm[pl.ds(r, 1), :], (8, L))
            new = [[None] * halves for _ in range(6)]
            for c in range(6):
                before = jnp.broadcast_to(gb[c, pl.ds(r, 1), :], (8, L))
                for t in range(halves):
                    rows = slice(8 * t, 8 * t + 8)
                    lines = [
                        Line(lambda i, g=g: vd[g, c, 8 * t + 3 + i : 8 * t + 11 + i],
                             lambda i, g=g: vs[g, c, 8 * t + 3 + i : 8 * t + 11 + i])
                        for g in range(1 if c in ZERO[1] else 2)
                    ]
                    here = slice(8 * t + 3, 8 * t + 11)
                    double = None if c in ZERO[1] else vt[0, c, here] + vt[1, c, here]
                    f = face(lines[0], lines[1] if len(lines) > 1 else None, double)
                    turned = pltpu.roll(f, 1, 0)
                    lower = jnp.where(sub == 0, before, turned)
                    before = turned
                    patch = pltpu.roll(pd[c, t], lax.rem(L + L - 6 - slot * r, L), 1)
                    rate = jnp.where(edge, patch, acc[c, r, rows])
                    rate = rate + (cth[0, rows] * f - cth[1, rows] * lower)
                    rate = rate + (rp * fr[c, r + 1, rows] - rm * fr[c, r, rows])
                    new[c][t] = w * tile(0, c, r, t) + (1.0 - w) * (tile(stage, c, r, t) + rate)
            for t in range(halves):
                b, d = [new[c][t] for c in range(3)], [new[c][t] for c in range(3, 6)]
                b2 = jnp.maximum(b[0] * b[0] + b[1] * b[1] + b[2] * b[2], 1.0)
                along = (b[0] * d[0] + b[1] * d[1] + b[2] * d[2]) / b2
                d = [y - along * x for x, y in zip(b, d)]
                d2 = d[0] * d[0] + d[1] * d[1] + d[2] * d[2]
                shrink = jnp.sqrt(b2 / jnp.maximum(d2, b2))
                for c in range(3):
                    new[3 + c][t] = d[c] * shrink
                for c in range(6):
                    u[stage + 1, c, base + r, 8 * t : 8 * t + 8] = new[c][t]

            @pl.when(stage < 2)
            def _():
                pack(stage + 1, r, new)

            return carry

        lax.fori_loop(0, nr, final, 0)

        @pl.when(stage < 2)
        def _():
            send_all(stage + 1)

        return carry

    lax.fori_loop(0, 3, stage_body, 0)
    stores = [
        pltpu.make_async_copy(u.at[3, 3 * i : 3 * i + 3, base : base + nr, 0:nt], dst, local.at[i])
        for i, dst in enumerate((mag_out, ele_out))
    ]
    for c in stores:
        c.start()

    def drain(stage, carry):
        @pl.when(has_outer)
        def _():
            radial_out(stage).wait_send()

        @pl.when(has_inner)
        def _():
            radial_in(stage).wait_send()

        for c in theta_copies(stage) + phi_copies(stage):
            c.wait_send()
        return carry

    lax.fori_loop(0, 3, drain, 0)
    for c in stores:
        c.wait()


def solution(mesh):
    n_row, n_theta, n_phi = (mesh.shape[k] for k in ("row", "theta", "phi"))

    def body(magnetic, electric):
        _, nr, nt, lanes = magnetic.shape
        plane = -(-(nt + 2 * G) // 8) * 8
        planes = nr + 2 * G
        halves = nt // 8
        pad8 = lambda n: -(-n // 8) * 8
        f32 = jnp.float32
        vm = lambda *shape: pltpu.VMEM(shape, f32)
        sizes = (n_row, n_theta, n_phi, nr, nt, lanes, plane)
        anywhere = pl.BlockSpec(memory_space=pl.ANY)
        packs = vm(3, 6, halves, 8, lanes)
        joined = vm(3, 2, halves, 8, lanes)
        return pl.pallas_call(
            functools.partial(kernel, sizes),
            out_shape=[jax.ShapeDtypeStruct(magnetic.shape, f32)] * 2,
            in_specs=[anywhere] * 2,
            out_specs=[anywhere] * 2,
            scratch_shapes=[
                vm(4, 6, planes + 2, plane, lanes),
                packs, packs,
                joined, joined, joined, joined,
                vm(3, 2, 6 * G * nr, lanes),
                vm(3, 2, 6 * G * nr, lanes),
                vm(6, nr + 1, nt, lanes),
                vm(6, nr, nt, lanes),
                vm(2, 6, planes, nt, lanes),
                vm(2, 6, nt + 16, lanes),
                vm(2, 6, nt + 16, lanes),
                vm(2, 6, nt + 16, lanes),
                vm(6, pad8(nr), lanes),
                vm(6, halves, 8, lanes),
                vm(pad8(planes), lanes),
                vm(pad8(planes), lanes),
                vm(pad8(nr), lanes),
                vm(pad8(nr), lanes),
                vm(2, nt, lanes),
                pltpu.SemaphoreType.DMA((3, 6)),
                pltpu.SemaphoreType.DMA((3, 6)),
                pltpu.SemaphoreType.DMA((2,)),
            ],
            compiler_params=pltpu.CompilerParams(
                collective_id=0, has_side_effects=True, vmem_limit_bytes=24 * 1024 * 1024
            ),
        )(magnetic, electric)

    spec = P(None, "row", "theta", "phi")
    return jax.shard_map(body, mesh=mesh, in_specs=(spec, spec), out_specs=(spec, spec), check_vma=False)
```

```python
import functools
import math

import jax
import jax.numpy as jnp
from jax import lax
from jax.experimental import pallas as pl
from jax.experimental.pallas import tpu as pltpu
from jax.sharding import PartitionSpec as P

MESH = pl.DeviceIdType.MESH
hole_mass = 1.0
inner_radius = 1.8
wave_speed = 1.25
courant = 0.3
smooth_eps = 1e-06
G = 3
ZERO = ((0, 3), (1, 4), (2, 5))


def flux_of(dim, u, a, s):
    b1, b2, b3, d1, d2, d3 = u
    if dim == 0:
        e2, e3 = a * d2 - s * b3, a * d3 + s * b2
        h2, h3 = a * b2 + s * d3, a * b3 - s * d2
        return [None, -e3, e2, None, h3, -h2]
    if dim == 1:
        e1, e3 = a * d1, a * d3 + s * b2
        h1, h3 = a * b1, a * b3 - s * d2
        return [e3, None, -e1, -h3, None, h1]
    e1, e2 = a * d1, a * d2 - s * b3
    h1, h2 = a * b1, a * b2 + s * d3
    return [-e2, e1, None, h2, -h1, None]


def split(dim, u, a, s):
    out = []
    for f, x in zip(flux_of(dim, u, a, s), u):
        k = wave_speed * x
        out.append((k, -k) if f is None else (f + k, f - k))
    return out


class Line:
    def __init__(self, d, r=None, t3=None):
        self.made, self.d0, self.r0, self.t0 = {}, d, r, t3

    def keep(self, kind, i, make):
        if (kind, i) not in self.made:
            self.made[kind, i] = make()
        return self.made[kind, i]

    def d(self, i):
        return self.keep(0, i, lambda: self.d0(i))

    def square(self, i):
        k, eps = 0.609375, 3.0 * smooth_eps
        return (k * self.d(i)) * self.d(i) + eps

    def r(self, i):
        return self.keep(1, i, lambda: self.r0(i) if self.r0 else self.square(i))

    def q(self, i):
        return self.keep(2, i, lambda: 1.375 * self.d(i))

    def h(self, i):
        return self.keep(3, i, lambda: 0.625 * self.d(i))

    def step(self, i):
        return self.keep(4, i, lambda: self.d(i) - self.d(i - 1))

    def third(self, i):
        return self.step(i + 1) - self.step(i)

    def t(self, i):
        return self.keep(5, i, lambda: self.t0(i) if self.t0 else self.third(i))


def correction(line, i, way):
    i0, i1, i3 = i - 2 * way, i - way, i + way
    x0 = line.d(i0) - line.q(i1)
    x1 = line.d(i1) - line.h(i)
    x2 = line.d(i3) - line.q(i)
    s0, s1, s2 = x0 * x0 + line.r(i1), x1 * x1 + line.r(i), x2 * x2 + line.r(i)
    s0, s1, s2 = s0 * s0, s1 * s1, s2 * s2
    z = 3.0 * s0
    n0, n2, y = s1 * s2, z * s1, z * s2
    den = (n0 + n2) + (y + y)
    return ((n0 + n0) * line.t(i1) + n2 * line.t(i)) * pl.reciprocal(den, approx=True)


def face(p, m, double, i=0):
    if m is None:
        return p.t(i) - (correction(p, i, 1) + correction(p, i, -1))
    dm = m.d(i)
    lin = 6.0 * double + ((p.d(i - 1) - m.d(i + 1)) + 2.0 * (p.d(i) + (dm + dm)))
    return lin - (correction(p, i, 1) - correction(m, i, -1))


def line_of(values, start=0):
    return Line(lambda i: values[i + 1 - start] - values[i - start])


def kernel(sizes, mag, ele, mag_out, ele_out, u, pa, pb, sa, sb, ra, rb, te0, te1, tr0, tr1, fr, acc, vr, vt, vd, vs, gb, pd,
           ca, cs, crp, crm, cth, send, recv, local):
    n_row, n_theta, n_phi, nr, nt, L, plane = sizes
    row, th, ph = lax.axis_index("row"), lax.axis_index("theta"), lax.axis_index("phi")
    slot = L // nr
    halves = nt // 8
    spacing = math.pi / (nt * n_theta)
    spacing_phi = 2.0 * math.pi / (L * n_phi)
    dt = courant / (1.0 / spacing + 1.0 / spacing + 1.0 / spacing_phi)
    scale = -dt / 12.0
    planes = nr + 2 * G
    flat = u.reshape(u.shape[0], 6, (planes + 2) * plane, L)
    first, last = th == 0, th == n_theta - 1
    opposite = (row, th, lax.rem(ph + n_phi // 2, n_phi))
    right = (row, th, lax.rem(ph + 1, n_phi))
    left = (row, th, lax.rem(ph + n_phi - 1, n_phi))
    above = tuple(jnp.where(last, o, q) for o, q in zip(opposite, (row, th + 1, ph)))
    below = tuple(jnp.where(first, o, q) for o, q in zip(opposite, (row, th - 1, ph)))
    outer, inner = (row + 1, th, ph), (row - 1, th, ph)
    has_outer, has_inner = row < n_row - 1, row > 0

    loads = [
        pltpu.make_async_copy(src, u.at[0, 3 * i : 3 * i + 3, 1 + G : 1 + G + nr, 0:nt], local.at[i])
        for i, src in enumerate((mag, ele))
    ]
    for c in loads:
        c.start()

    barrier = pltpu.get_barrier_semaphore()
    for target in (above, below, right, left):
        pl.semaphore_signal(barrier, inc=1, device_id=target, device_id_type=MESH)

    @pl.when(has_outer)
    def _():
        pl.semaphore_signal(barrier, inc=1, device_id=outer, device_id_type=MESH)

    @pl.when(has_inner)
    def _():
        pl.semaphore_signal(barrier, inc=1, device_id=inner, device_id_type=MESH)

    lane = lax.broadcasted_iota(jnp.int32, (8, L), 1)
    sub = lax.broadcasted_iota(jnp.int32, (8, L), 0)
    owner = jnp.zeros((8, L), jnp.int32)
    for q in range(1, nr):
        owner = owner + (lane >= slot * q).astype(jnp.int32)
    in_slot = lane - slot * owner

    def radius_at(index):
        return inner_radius + (index.astype(jnp.float32) + 0.5) * spacing

    def lapse_shift(radius):
        ratio = 2.0 * hole_mass / radius
        return 1.0 / jnp.sqrt(1.0 + ratio), ratio / (1.0 + ratio)

    for q in range(ca.shape[0] // 8):
        a, s = lapse_shift(radius_at(row * nr - G + 8 * q + sub))
        ca[8 * q : 8 * q + 8] = a
        cs[8 * q : 8 * q + 8] = s
    for q in range(crp.shape[0] // 8):
        index = row * nr + 8 * q + sub
        rc, hi, lo = radius_at(index), radius_at(index + 1), radius_at(index - 1)
        crp[8 * q : 8 * q + 8] = scale * (0.5 * (rc + hi)) ** 2 / (rc * rc * spacing)
        crm[8 * q : 8 * q + 8] = scale * (0.5 * (rc + lo)) ** 2 / (rc * rc * spacing)
    for q in range(halves):
        index = (th * nt + 8 * q + sub).astype(jnp.float32)
        mid = jnp.sin((index + 0.5) * spacing)
        cth[0, 8 * q : 8 * q + 8] = scale * jnp.sin((index + 1.0) * spacing) / (mid * spacing)
        cth[1, 8 * q : 8 * q + 8] = scale * jnp.sin(index * spacing) / (mid * spacing)
    a_lane, s_lane = lapse_shift(radius_at(row * nr + owner))
    coef_phi = scale / spacing_phi

    zeros = jnp.zeros((nt, L), jnp.float32)
    for stage in range(3):
        @pl.when(row == 0)
        def _():
            for c in range(6):
                for q in range(G):
                    u[stage, c, 1 + q, 0:nt] = zeros

        @pl.when(row == n_row - 1)
        def _():
            for c in range(6):
                for q in range(G):
                    u[stage, c, 1 + G + nr + q, 0:nt] = zeros

    def pack(stage, r, tiles):
        mask = (lane >= slot * r) & (lane < slot * r + slot)
        for c in range(6):
            for t in range(halves):
                x = tiles[c][t]
                pa[stage, c, t] = jnp.where(mask, pltpu.roll(x, slot * r + 3, 1), pa[stage, c, t])
                pb[stage, c, t] = jnp.where(
                    mask, pltpu.roll(x, lax.rem(slot * r + 6, L), 1), pb[stage, c, t]
                )

    def tile(stage, c, r, t):
        return u[stage, c, 1 + G + r, 8 * t : 8 * t + 8]

    def remote(src, dst, stage, m_send, m_recv, target):
        return pltpu.make_async_remote_copy(
            src_ref=src, dst_ref=dst, send_sem=send.at[stage, m_send], recv_sem=recv.at[stage, m_recv],
            device_id=target, device_id_type=MESH,
        )

    base = 1 + G

    def radial_out(stage):
        return remote(u.at[stage, :, base + nr - G : base + nr, 0:nt], u.at[stage, :, 1 : 1 + G, 0:nt],
                      stage, 0, 0, outer)

    def radial_in(stage):
        return remote(u.at[stage, :, base : base + G, 0:nt],
                      u.at[stage, :, base + nr : base + nr + G, 0:nt], stage, 1, 1, inner)

    def theta_copies(stage, part):
        up = jnp.where(last, 1, 0)
        down = jnp.where(first, 0, 1)
        te, tr = (te0, te1)[part], (tr0, tr1)[part]
        n = 2 + 4 * part
        return (
            remote(te.at[stage, 1], tr.at[stage, up], stage, n, n + up, above),
            remote(te.at[stage, 0], tr.at[stage, down], stage, n + 1, n + down, below),
        )

    def phi_copies(stage):
        return (
            remote(sa.at[stage], ra.at[stage], stage, 4, 4, right),
            remote(sb.at[stage], rb.at[stage], stage, 5, 5, left),
        )

    starts = list(range(0, nr - 7, 8))
    if starts[-1] + 8 < nr:
        starts.append(nr - 8)

    def grab(stage, c, r0, k):
        return flat[stage, c, pl.ds((base + r0) * plane + k, 8, stride=plane), :]

    def row_of(q):
        return jnp.where(q < G, q, jnp.where(q < 2 * G, q + nr - 2 * G, q - G))

    def send_radial(stage):
        @pl.when(has_outer)
        def _():
            radial_out(stage).start()

        @pl.when(has_inner)
        def _():
            radial_in(stage).start()

    def send_theta(stage, part):
        te = (te0, te1)[part]

        def gather(q, carry):
            top = (base + row_of(q + 2 * G * part)) * plane
            for side in range(2):
                for c in range(6):
                    x = flat[stage, c, pl.ds(top + (nt - G) * side, G), :]
                    te[stage, side, pl.ds((q * 6 + c) * G, G), :] = x
            return carry

        lax.fori_loop(0, (2 * G, nr - 2 * G)[part], gather, 0)
        for c in theta_copies(stage, part):
            c.start()

    def send_phi(stage):
        for g in range(2):
            for t in range(halves):
                x, y = pa[stage, 3 * g + 1, t], pa[stage, 3 * g + 2, t]
                x = jnp.where(in_slot < 6, pltpu.roll(x, 3, 1), pltpu.roll(y, 6, 1))
                sa[stage, g, t] = jnp.where(in_slot < 3, pa[stage, 3 * g, t], x)
                x, y = pb[stage, 3 * g + 1, t], pb[stage, 3 * g + 2, t]
                x = jnp.where(in_slot < 3, pltpu.roll(y, L - 6, 1), pltpu.roll(x, L - 3, 1))
                sb[stage, g, t] = jnp.where(in_slot < 6, x, pb[stage, 3 * g, t])
        for c in phi_copies(stage):
            c.start()

    for c in loads:
        c.wait()

    pl.semaphore_wait(barrier, 4 + jnp.where(has_outer, 1, 0) + jnp.where(has_inner, 1, 0))
    send_radial(0)
    for part in range(2):
        send_theta(0, part)

    def pack_first(r, carry):
        pack(0, r, [[tile(0, c, r, t) for t in range(halves)] for c in range(6)])
        return carry

    lax.fori_loop(0, nr, pack_first, 0)
    send_phi(0)

    def rolled(v, k):
        return v if k == 0 else pltpu.roll(v, (-k) % L, 1)

    def turning(v):
        made = {}

        def at(kind, i, make):
            if i == 0:
                if kind not in made:
                    made[kind] = make()
                return made[kind]
            return rolled(at(kind, 0, make), i)

        line = Line(
            lambda i: at(0, i, lambda: rolled(v, 1) - v),
            lambda i: at(1, i, lambda: line.square(0)),
            lambda i: at(2, i, lambda: line.third(0)),
        )
        return line

    def phi_div(split_values):
        out = []
        for c, (vp, vm) in enumerate(split_values):
            f = face(turning(vp), None if c in ZERO[2] else turning(vm), vp + vm)
            out.append(coef_phi * (f - pltpu.roll(f, 1, 1)))
        return out

    def coefs(p):
        return (
            jnp.broadcast_to(ca[pl.ds(p, 1), :], (8, L)),
            jnp.broadcast_to(cs[pl.ds(p, 1), :], (8, L)),
        )

    def stage_body(stage, carry):
        def phi_pass(r, carry):
            a, s = coefs(r + G)
            for t in range(halves):
                x = [tile(stage, c, r, t) for c in range(6)]
                for c, d in enumerate(phi_div(split(2, x, a, s))):
                    acc[c, r, 8 * t : 8 * t + 8] = d
                for c, (vp, vm) in enumerate(split(0, x, a, s)):
                    vr[0, c, r + G, 8 * t : 8 * t + 8] = vp
                    vr[1, c, r + G, 8 * t : 8 * t + 8] = vm
            return carry

        lax.fori_loop(0, nr, phi_pass, 0)

        def radial_faces(lo, hi):
            def part(t, carry):
                rows = pl.ds(pl.multiple_of(8 * t, 8), 8)
                for c in range(6):
                    p = [vr[0, c, k, rows] for k in range(lo, hi + 5)]
                    pline, mline, m = line_of(p, lo), None, None
                    if c not in ZERO[0]:
                        m = [vr[1, c, k, rows] for k in range(lo, hi + 5)]
                        mline = line_of(m, lo)
                    for f in range(lo, hi):
                        i = f + 2
                        double = None if m is None else p[i - lo] + m[i - lo]
                        fr[c, f, rows] = face(pline, mline, double, i)
                return carry

            lax.fori_loop(0, halves, part, 0)

        radial_faces(G, nr - G + 1)

        @pl.when(has_inner)
        def _():
            radial_out(stage).wait_recv()

        @pl.when(has_outer)
        def _():
            radial_in(stage).wait_recv()

        def ghost_planes(q, carry):
            p = jnp.where(q < G, q, q + nr)
            a, s = coefs(p)
            for t in range(halves):
                x = [u[stage, c, 1 + p, 8 * t : 8 * t + 8] for c in range(6)]
                for c, (vp, vm) in enumerate(split(0, x, a, s)):
                    vr[0, c, p, 8 * t : 8 * t + 8] = vp
                    vr[1, c, p, 8 * t : 8 * t + 8] = vm
            return carry

        lax.fori_loop(0, 2 * G, ghost_planes, 0)

        radial_faces(0, G)
        radial_faces(nr - G + 1, nr + 1)

        for part in range(2):
            te, tr = (te0, te1)[part], (tr0, tr1)[part]
            for side in range(2):
                remote(te.at[stage, side], tr.at[stage, side], stage, 2, 2 + 4 * part + side, above).wait_recv()

            def scatter(q, carry):
                top = (base + row_of(q + 2 * G * part)) * plane
                for side in range(2):
                    pole = first if side == 0 else last
                    sign = jnp.where(pole, -1.0, 1.0)
                    for g in range(G):
                        k = jnp.where(pole, G - 1 - g, g)
                        for c in range(6):
                            x = tr[stage, side, pl.ds((q * 6 + c) * G + k, 1), :]
                            if c % 3:
                                x = x * sign
                            flat[stage, c, pl.ds(top + (g - G if side == 0 else nt + g), 1), :] = x
                return carry

            lax.fori_loop(0, (2 * G, nr - 2 * G)[part], scatter, 0)

        for r0 in starts:
            a, s = ca[G + r0 : G + r0 + 8], cs[G + r0 : G + r0 + 8]
            v = [split(1, [grab(stage, c, r0, k) for c in range(6)], a, s) for k in range(-3, 3)]
            for c in range(6):
                pline = line_of([v[k][c][0] for k in range(6)], -2)
                mline = None if c in ZERO[1] else line_of([v[k][c][1] for k in range(6)], -2)
                gb[c, r0 : r0 + 8] = face(pline, mline, v[2][c][0] + v[2][c][1])

        for c in phi_copies(stage):
            c.wait_recv()

        def packed(t, carry):
            xa = [
                jnp.where(in_slot < 3, rolled(ra[stage, c // 3, t], 3 * (c % 3)), pa[stage, c, t])
                for c in range(6)
            ]
            xb = [
                jnp.where(in_slot >= 6, rolled(rb[stage, c // 3, t], -3 * (c % 3)), pb[stage, c, t])
                for c in range(6)
            ]
            da = phi_div(split(2, xa, a_lane, s_lane))
            db = phi_div(split(2, xb, a_lane, s_lane))
            for c in range(6):
                pd[c, t] = jnp.where(in_slot < 6, db[c], pltpu.roll(da[c], 3, 1))
            return carry

        lax.fori_loop(0, halves, packed, 0)

        w = jnp.where(stage == 0, 0.0, jnp.where(stage == 1, 0.75, 1.0 / 3.0)).astype(jnp.float32)
        edge = (lane < 3) | (lane >= L - 3)

        def final(q, carry):
            r = row_of(q)
            a, s = coefs(r + G)
            top = (base + r) * plane - G
            for o in range(halves + 1):
                x = [flat[stage, c, pl.ds(top + 8 * o, 8), :] for c in range(6)]
                for c, values in enumerate(split(1, x, a, s)):
                    for sign, v in enumerate(values):
                        vt[sign, c, 8 * o : 8 * o + 8] = v
            for c in range(6):
                for sign in range(1 if c in ZERO[1] else 2):
                    for o in range(halves + 1):
                        d = vt[sign, c, 8 * o + 1 : 8 * o + 9] - vt[sign, c, 8 * o : 8 * o + 8]
                        vd[sign, c, 8 * o : 8 * o + 8] = d
                        vs[sign, c, 8 * o : 8 * o + 8] = Line(lambda i: d).square(0)
            rp = jnp.broadcast_to(crp[pl.ds(r, 1), :], (8, L))
            rm = jnp.broadcast_to(crm[pl.ds(r, 1), :], (8, L))
            new = [[None] * halves for _ in range(6)]
            for c in range(6):
                before = jnp.broadcast_to(gb[c, pl.ds(r, 1), :], (8, L))
                for t in range(halves):
                    rows = slice(8 * t, 8 * t + 8)
                    lines = [
                        Line(lambda i, g=g: vd[g, c, 8 * t + 3 + i : 8 * t + 11 + i],
                             lambda i, g=g: vs[g, c, 8 * t + 3 + i : 8 * t + 11 + i])
                        for g in range(1 if c in ZERO[1] else 2)
                    ]
                    here = slice(8 * t + 3, 8 * t + 11)
                    double = None if c in ZERO[1] else vt[0, c, here] + vt[1, c, here]
                    f = face(lines[0], lines[1] if len(lines) > 1 else None, double)
                    turned = pltpu.roll(f, 1, 0)
                    lower = jnp.where(sub == 0, before, turned)
                    before = turned
                    patch = pltpu.roll(pd[c, t], lax.rem(L + L - 6 - slot * r, L), 1)
                    rate = jnp.where(edge, patch, acc[c, r, rows])
                    rate = rate + (cth[0, rows] * f - cth[1, rows] * lower)
                    rate = rate + (rp * fr[c, r + 1, rows] - rm * fr[c, r, rows])
                    new[c][t] = w * tile(0, c, r, t) + (1.0 - w) * (tile(stage, c, r, t) + rate)
            for t in range(halves):
                b, d = [new[c][t] for c in range(3)], [new[c][t] for c in range(3, 6)]
                b2 = jnp.maximum(b[0] * b[0] + b[1] * b[1] + b[2] * b[2], 1.0)
                along = (b[0] * d[0] + b[1] * d[1] + b[2] * d[2]) / b2
                d = [y - along * x for x, y in zip(b, d)]
                d2 = d[0] * d[0] + d[1] * d[1] + d[2] * d[2]
                shrink = jnp.sqrt(b2 / jnp.maximum(d2, b2))
                for c in range(3):
                    new[3 + c][t] = d[c] * shrink
                for c in range(6):
                    u[stage + 1, c, base + r, 8 * t : 8 * t + 8] = new[c][t]

            @pl.when(stage < 2)
            def _():
                pack(stage + 1, r, new)

            return carry

        lax.fori_loop(0, 2 * G, final, 0)

        @pl.when(stage < 2)
        def _():
            send_radial(stage + 1)
            send_theta(stage + 1, 0)

        lax.fori_loop(2 * G, nr, final, 0)

        @pl.when(stage < 2)
        def _():
            send_theta(stage + 1, 1)
            send_phi(stage + 1)

        return carry

    lax.fori_loop(0, 3, stage_body, 0)
    stores = [
        pltpu.make_async_copy(u.at[3, 3 * i : 3 * i + 3, base : base + nr, 0:nt], dst, local.at[i])
        for i, dst in enumerate((mag_out, ele_out))
    ]
    for c in stores:
        c.start()

    def drain(stage, carry):
        @pl.when(has_outer)
        def _():
            radial_out(stage).wait_send()

        @pl.when(has_inner)
        def _():
            radial_in(stage).wait_send()

        for c in theta_copies(stage, 0) + theta_copies(stage, 1) + phi_copies(stage):
            c.wait_send()
        return carry

    lax.fori_loop(0, 3, drain, 0)
    for c in stores:
        c.wait()


def solution(mesh):
    n_row, n_theta, n_phi = (mesh.shape[k] for k in ("row", "theta", "phi"))

    def body(magnetic, electric):
        _, nr, nt, lanes = magnetic.shape
        plane = -(-(nt + 2 * G) // 8) * 8
        planes = nr + 2 * G
        halves = nt // 8
        pad8 = lambda n: -(-n // 8) * 8
        f32 = jnp.float32
        vm = lambda *shape: pltpu.VMEM(shape, f32)
        sizes = (n_row, n_theta, n_phi, nr, nt, lanes, plane)
        anywhere = pl.BlockSpec(memory_space=pl.ANY)
        packs = vm(3, 6, halves, 8, lanes)
        edges = lambda n: vm(3, 2, 6 * G * n, lanes)
        joined = vm(3, 2, halves, 8, lanes)
        return pl.pallas_call(
            functools.partial(kernel, sizes),
            out_shape=[jax.ShapeDtypeStruct(magnetic.shape, f32)] * 2,
            in_specs=[anywhere] * 2,
            out_specs=[anywhere] * 2,
            scratch_shapes=[
                vm(4, 6, planes + 2, plane, lanes),
                packs, packs,
                joined, joined, joined, joined,
                edges(2 * G), edges(nr - 2 * G),
                edges(2 * G), edges(nr - 2 * G),
                vm(6, nr + 1, nt, lanes),
                vm(6, nr, nt, lanes),
                vm(2, 6, planes, nt, lanes),
                vm(2, 6, nt + 16, lanes),
                vm(2, 6, nt + 16, lanes),
                vm(2, 6, nt + 16, lanes),
                vm(6, pad8(nr), lanes),
                vm(6, halves, 8, lanes),
                vm(pad8(planes), lanes),
                vm(pad8(planes), lanes),
                vm(pad8(nr), lanes),
                vm(pad8(nr), lanes),
                vm(2, nt, lanes),
                pltpu.SemaphoreType.DMA((3, 8)),
                pltpu.SemaphoreType.DMA((3, 8)),
                pltpu.SemaphoreType.DMA((2,)),
            ],
            compiler_params=pltpu.CompilerParams(
                collective_id=0, has_side_effects=True
            ),
        )(magnetic, electric)

    spec = P(None, "row", "theta", "phi")
    return jax.shard_map(body, mesh=mesh, in_specs=(spec, spec), out_specs=(spec, spec), check_vma=False)
```

```python
import functools
import math

import jax
import jax.numpy as jnp
from jax import lax
from jax.experimental import pallas as pl
from jax.experimental.pallas import tpu as pltpu
from jax.sharding import PartitionSpec as P

MESH = pl.DeviceIdType.MESH
hole_mass = 1.0
inner_radius = 1.8
wave_speed = 1.25
courant = 0.3
smooth_eps = 1e-06
G = 3
ZERO = ((0, 3), (1, 4), (2, 5))


def flux_of(dim, u, a, s):
    b1, b2, b3, d1, d2, d3 = u
    if dim == 0:
        e2, e3 = a * d2 - s * b3, a * d3 + s * b2
        h2, h3 = a * b2 + s * d3, a * b3 - s * d2
        return [None, -e3, e2, None, h3, -h2]
    if dim == 1:
        e1, e3 = a * d1, a * d3 + s * b2
        h1, h3 = a * b1, a * b3 - s * d2
        return [e3, None, -e1, -h3, None, h1]
    e1, e2 = a * d1, a * d2 - s * b3
    h1, h2 = a * b1, a * b2 + s * d3
    return [-e2, e1, None, h2, -h1, None]


def split(dim, u, a, s):
    out = []
    for f, x in zip(flux_of(dim, u, a, s), u):
        k = wave_speed * x
        out.append((k, -k) if f is None else (f + k, f - k))
    return out


class Line:
    def __init__(self, d, r=None, t3=None):
        self.made, self.d0, self.r0, self.t0 = {}, d, r, t3

    def keep(self, kind, i, make):
        if (kind, i) not in self.made:
            self.made[kind, i] = make()
        return self.made[kind, i]

    def d(self, i):
        return self.keep(0, i, lambda: self.d0(i))

    def square(self, i):
        k, eps = 0.609375, 3.0 * smooth_eps
        return (k * self.d(i)) * self.d(i) + eps

    def r(self, i):
        return self.keep(1, i, lambda: self.r0(i) if self.r0 else self.square(i))

    def q(self, i):
        return self.keep(2, i, lambda: 1.375 * self.d(i))

    def h(self, i):
        return self.keep(3, i, lambda: 0.625 * self.d(i))

    def step(self, i):
        return self.keep(4, i, lambda: self.d(i) - self.d(i - 1))

    def third(self, i):
        return self.step(i + 1) - self.step(i)

    def t(self, i):
        return self.keep(5, i, lambda: self.t0(i) if self.t0 else self.third(i))


def correction(line, i, way):
    i0, i1, i3 = i - 2 * way, i - way, i + way
    x0 = line.d(i0) - line.q(i1)
    x1 = line.d(i1) - line.h(i)
    x2 = line.d(i3) - line.q(i)
    s0, s1, s2 = x0 * x0 + line.r(i1), x1 * x1 + line.r(i), x2 * x2 + line.r(i)
    s0, s1, s2 = s0 * s0, s1 * s1, s2 * s2
    z = 3.0 * s0
    n0, n2, y = s1 * s2, z * s1, z * s2
    den = (n0 + n2) + (y + y)
    return ((n0 + n0) * line.t(i1) + n2 * line.t(i)) * pl.reciprocal(den, approx=True)


def face(p, m, double, i=0):
    if m is None:
        return p.t(i) - (correction(p, i, 1) + correction(p, i, -1))
    dm = m.d(i)
    lin = 6.0 * double + ((p.d(i - 1) - m.d(i + 1)) + 2.0 * (p.d(i) + (dm + dm)))
    return lin - (correction(p, i, 1) - correction(m, i, -1))


def line_of(values, start=0):
    return Line(lambda i: values[i + 1 - start] - values[i - start])


def kernel(sizes, mag, ele, mag_out, ele_out, u, pa, pb, sa, sb, ra, rb, te, tr, fr, acc, vr, vt, vd, vs, gb, pd,
           ca, cs, crp, crm, cth, send, recv, local):
    n_row, n_theta, n_phi, nr, nt, L, plane = sizes
    row, th, ph = lax.axis_index("row"), lax.axis_index("theta"), lax.axis_index("phi")
    slot = L // nr
    halves = nt // 8
    spacing = math.pi / (nt * n_theta)
    spacing_phi = 2.0 * math.pi / (L * n_phi)
    dt = courant / (1.0 / spacing + 1.0 / spacing + 1.0 / spacing_phi)
    scale = -dt / 12.0
    planes = nr + 2 * G
    flat = u.reshape(u.shape[0], 6, (planes + 2) * plane, L)
    first, last = th == 0, th == n_theta - 1
    opposite = (row, th, lax.rem(ph + n_phi // 2, n_phi))
    right = (row, th, lax.rem(ph + 1, n_phi))
    left = (row, th, lax.rem(ph + n_phi - 1, n_phi))
    above = tuple(jnp.where(last, o, q) for o, q in zip(opposite, (row, th + 1, ph)))
    below = tuple(jnp.where(first, o, q) for o, q in zip(opposite, (row, th - 1, ph)))
    outer, inner = (row + 1, th, ph), (row - 1, th, ph)
    has_outer, has_inner = row < n_row - 1, row > 0

    loads = [
        pltpu.make_async_copy(src, u.at[0, 3 * i : 3 * i + 3, 1 + G : 1 + G + nr, 0:nt], local.at[i])
        for i, src in enumerate((mag, ele))
    ]
    for c in loads:
        c.start()

    barrier = pltpu.get_barrier_semaphore()
    for target in (above, below, right, left):
        pl.semaphore_signal(barrier, inc=1, device_id=target, device_id_type=MESH)

    @pl.when(has_outer)
    def _():
        pl.semaphore_signal(barrier, inc=1, device_id=outer, device_id_type=MESH)

    @pl.when(has_inner)
    def _():
        pl.semaphore_signal(barrier, inc=1, device_id=inner, device_id_type=MESH)

    lane = lax.broadcasted_iota(jnp.int32, (8, L), 1)
    sub = lax.broadcasted_iota(jnp.int32, (8, L), 0)
    owner = jnp.zeros((8, L), jnp.int32)
    for q in range(1, nr):
        owner = owner + (lane >= slot * q).astype(jnp.int32)
    in_slot = lane - slot * owner

    def radius_at(index):
        return inner_radius + (index.astype(jnp.float32) + 0.5) * spacing

    def lapse_shift(radius):
        ratio = 2.0 * hole_mass / radius
        return 1.0 / jnp.sqrt(1.0 + ratio), ratio / (1.0 + ratio)

    for q in range(ca.shape[0] // 8):
        a, s = lapse_shift(radius_at(row * nr - G + 8 * q + sub))
        ca[8 * q : 8 * q + 8] = a
        cs[8 * q : 8 * q + 8] = s
    for q in range(crp.shape[0] // 8):
        index = row * nr + 8 * q + sub
        rc, hi, lo = radius_at(index), radius_at(index + 1), radius_at(index - 1)
        crp[8 * q : 8 * q + 8] = scale * (0.5 * (rc + hi)) ** 2 / (rc * rc * spacing)
        crm[8 * q : 8 * q + 8] = scale * (0.5 * (rc + lo)) ** 2 / (rc * rc * spacing)
    for q in range(halves):
        index = (th * nt + 8 * q + sub).astype(jnp.float32)
        mid = jnp.sin((index + 0.5) * spacing)
        cth[0, 8 * q : 8 * q + 8] = scale * jnp.sin((index + 1.0) * spacing) / (mid * spacing)
        cth[1, 8 * q : 8 * q + 8] = scale * jnp.sin(index * spacing) / (mid * spacing)
    a_lane, s_lane = lapse_shift(radius_at(row * nr + owner))
    coef_phi = scale / spacing_phi

    zeros = jnp.zeros((nt, L), jnp.float32)
    for stage in range(3):
        @pl.when(row == 0)
        def _():
            for c in range(6):
                for q in range(G):
                    u[stage, c, 1 + q, 0:nt] = zeros

        @pl.when(row == n_row - 1)
        def _():
            for c in range(6):
                for q in range(G):
                    u[stage, c, 1 + G + nr + q, 0:nt] = zeros

    def pack(stage, r, tiles):
        mask = (lane >= slot * r) & (lane < slot * r + slot)
        for c in range(6):
            for t in range(halves):
                x = tiles[c][t]
                pa[stage, c, t] = jnp.where(mask, pltpu.roll(x, slot * r + 3, 1), pa[stage, c, t])
                pb[stage, c, t] = jnp.where(
                    mask, pltpu.roll(x, lax.rem(slot * r + 6, L), 1), pb[stage, c, t]
                )

    def tile(stage, c, r, t):
        return u[stage, c, 1 + G + r, 8 * t : 8 * t + 8]

    def remote(src, dst, stage, m_send, m_recv, target):
        return pltpu.make_async_remote_copy(
            src_ref=src, dst_ref=dst, send_sem=send.at[stage, m_send], recv_sem=recv.at[stage, m_recv],
            device_id=target, device_id_type=MESH,
        )

    base = 1 + G

    def radial_out(stage):
        return remote(u.at[stage, :, base + nr - G : base + nr, 0:nt], u.at[stage, :, 1 : 1 + G, 0:nt],
                      stage, 0, 0, outer)

    def radial_in(stage):
        return remote(u.at[stage, :, base : base + G, 0:nt],
                      u.at[stage, :, base + nr : base + nr + G, 0:nt], stage, 1, 1, inner)

    def theta_copies(stage):
        up = jnp.where(last, 1, 0)
        down = jnp.where(first, 0, 1)
        return (
            remote(te.at[stage, 1], tr.at[stage, up], stage, 2, 2 + up, above),
            remote(te.at[stage, 0], tr.at[stage, down], stage, 3, 2 + down, below),
        )

    def phi_copies(stage):
        return (
            remote(sa.at[stage], ra.at[stage], stage, 4, 4, right),
            remote(sb.at[stage], rb.at[stage], stage, 5, 5, left),
        )

    starts = list(range(0, nr - 7, 8))
    if starts[-1] + 8 < nr:
        starts.append(nr - 8)

    def grab(stage, c, r0, k):
        return flat[stage, c, pl.ds((base + r0) * plane + k, 8, stride=plane), :]

    def send_all(stage):
        @pl.when(has_outer)
        def _():
            radial_out(stage).start()

        @pl.when(has_inner)
        def _():
            radial_in(stage).start()

        for g in range(2):
            for t in range(halves):
                x, y = pa[stage, 3 * g + 1, t], pa[stage, 3 * g + 2, t]
                x = jnp.where(in_slot < 6, pltpu.roll(x, 3, 1), pltpu.roll(y, 6, 1))
                sa[stage, g, t] = jnp.where(in_slot < 3, pa[stage, 3 * g, t], x)
                x, y = pb[stage, 3 * g + 1, t], pb[stage, 3 * g + 2, t]
                x = jnp.where(in_slot < 3, pltpu.roll(y, L - 6, 1), pltpu.roll(x, L - 3, 1))
                sb[stage, g, t] = jnp.where(in_slot < 6, x, pb[stage, 3 * g, t])
        for side in range(2):
            for c in range(6):
                for k in range(G):
                    for r0 in starts:
                        te[stage, side, pl.ds((c * G + k) * nr + r0, 8), :] = grab(
                            stage, c, r0, k if side == 0 else nt - G + k
                        )
        for c in theta_copies(stage) + phi_copies(stage):
            c.start()

    for c in loads:
        c.wait()

    def pack_first(r, carry):
        pack(0, r, [[tile(0, c, r, t) for t in range(halves)] for c in range(6)])
        return carry

    lax.fori_loop(0, nr, pack_first, 0)
    pl.semaphore_wait(barrier, 4 + jnp.where(has_outer, 1, 0) + jnp.where(has_inner, 1, 0))
    send_all(0)

    def rolled(v, k):
        return v if k == 0 else pltpu.roll(v, (-k) % L, 1)

    def turning(v):
        made = {}

        def at(kind, i, make):
            if i == 0:
                if kind not in made:
                    made[kind] = make()
                return made[kind]
            return rolled(at(kind, 0, make), i)

        line = Line(
            lambda i: at(0, i, lambda: rolled(v, 1) - v),
            lambda i: at(1, i, lambda: line.square(0)),
            lambda i: at(2, i, lambda: line.third(0)),
        )
        return line

    def phi_div(split_values):
        out = []
        for c, (vp, vm) in enumerate(split_values):
            f = face(turning(vp), None if c in ZERO[2] else turning(vm), vp + vm)
            out.append(coef_phi * (f - pltpu.roll(f, 1, 1)))
        return out

    def coefs(p):
        return (
            jnp.broadcast_to(ca[pl.ds(p, 1), :], (8, L)),
            jnp.broadcast_to(cs[pl.ds(p, 1), :], (8, L)),
        )

    def stage_body(stage, carry):
        def phi_pass(r, carry):
            a, s = coefs(r + G)
            for t in range(halves):
                x = [tile(stage, c, r, t) for c in range(6)]
                for c, d in enumerate(phi_div(split(2, x, a, s))):
                    acc[c, r, 8 * t : 8 * t + 8] = d
                for c, (vp, vm) in enumerate(split(0, x, a, s)):
                    vr[0, c, r + G, 8 * t : 8 * t + 8] = vp
                    vr[1, c, r + G, 8 * t : 8 * t + 8] = vm
            return carry

        lax.fori_loop(0, nr, phi_pass, 0)

        def radial_faces(lo, hi):
            def part(t, carry):
                rows = pl.ds(pl.multiple_of(8 * t, 8), 8)
                for c in range(6):
                    p = [vr[0, c, k, rows] for k in range(lo, hi + 5)]
                    pline, mline, m = line_of(p, lo), None, None
                    if c not in ZERO[0]:
                        m = [vr[1, c, k, rows] for k in range(lo, hi + 5)]
                        mline = line_of(m, lo)
                    for f in range(lo, hi):
                        i = f + 2
                        double = None if m is None else p[i - lo] + m[i - lo]
                        fr[c, f, rows] = face(pline, mline, double, i)
                return carry

            lax.fori_loop(0, halves, part, 0)

        radial_faces(G, nr - G + 1)

        @pl.when(has_inner)
        def _():
            radial_out(stage).wait_recv()

        @pl.when(has_outer)
        def _():
            radial_in(stage).wait_recv()

        def ghost_planes(q, carry):
            p = jnp.where(q < G, q, q + nr)
            a, s = coefs(p)
            for t in range(halves):
                x = [u[stage, c, 1 + p, 8 * t : 8 * t + 8] for c in range(6)]
                for c, (vp, vm) in enumerate(split(0, x, a, s)):
                    vr[0, c, p, 8 * t : 8 * t + 8] = vp
                    vr[1, c, p, 8 * t : 8 * t + 8] = vm
            return carry

        lax.fori_loop(0, 2 * G, ghost_planes, 0)

        radial_faces(0, G)
        radial_faces(nr - G + 1, nr + 1)

        for side in range(2):
            remote(te.at[stage, side], tr.at[stage, side], stage, 2, 2 + side, above).wait_recv()
            pole = first if side == 0 else last
            sign = jnp.where(pole, -1.0, 1.0)
            for g in range(G):
                k = jnp.where(pole, G - 1 - g, g)
                for c in range(6):
                    for r0 in starts:
                        x = tr[stage, side, pl.ds((c * G + k) * nr + r0, 8), :]
                        if c % 3:
                            x = x * sign
                        target = (base + r0) * plane + (g - G if side == 0 else nt + g)
                        flat[stage, c, pl.ds(target, 8, stride=plane), :] = x

        for r0 in starts:
            a, s = ca[G + r0 : G + r0 + 8], cs[G + r0 : G + r0 + 8]
            v = [split(1, [grab(stage, c, r0, k) for c in range(6)], a, s) for k in range(-3, 3)]
            for c in range(6):
                pline = line_of([v[k][c][0] for k in range(6)], -2)
                mline = None if c in ZERO[1] else line_of([v[k][c][1] for k in range(6)], -2)
                gb[c, r0 : r0 + 8] = face(pline, mline, v[2][c][0] + v[2][c][1])

        for c in phi_copies(stage):
            c.wait_recv()

        def packed(t, carry):
            xa = [
                jnp.where(in_slot < 3, rolled(ra[stage, c // 3, t], 3 * (c % 3)), pa[stage, c, t])
                for c in range(6)
            ]
            xb = [
                jnp.where(in_slot >= 6, rolled(rb[stage, c // 3, t], -3 * (c % 3)), pb[stage, c, t])
                for c in range(6)
            ]
            da = phi_div(split(2, xa, a_lane, s_lane))
            db = phi_div(split(2, xb, a_lane, s_lane))
            for c in range(6):
                pd[c, t] = jnp.where(in_slot < 6, db[c], pltpu.roll(da[c], 3, 1))
            return carry

        lax.fori_loop(0, halves, packed, 0)

        w = jnp.where(stage == 0, 0.0, jnp.where(stage == 1, 0.75, 1.0 / 3.0)).astype(jnp.float32)
        edge = (lane < 3) | (lane >= L - 3)

        def final(r, carry):
            a, s = coefs(r + G)
            top = (base + r) * plane - G
            for q in range(halves + 1):
                x = [flat[stage, c, pl.ds(top + 8 * q, 8), :] for c in range(6)]
                for c, values in enumerate(split(1, x, a, s)):
                    for sign, v in enumerate(values):
                        vt[sign, c, 8 * q : 8 * q + 8] = v
            for c in range(6):
                for sign in range(1 if c in ZERO[1] else 2):
                    for q in range(halves + 1):
                        d = vt[sign, c, 8 * q + 1 : 8 * q + 9] - vt[sign, c, 8 * q : 8 * q + 8]
                        vd[sign, c, 8 * q : 8 * q + 8] = d
                        vs[sign, c, 8 * q : 8 * q + 8] = Line(lambda i: d).square(0)
            rp = jnp.broadcast_to(crp[pl.ds(r, 1), :], (8, L))
            rm = jnp.broadcast_to(crm[pl.ds(r, 1), :], (8, L))
            new = [[None] * halves for _ in range(6)]
            for c in range(6):
                before = jnp.broadcast_to(gb[c, pl.ds(r, 1), :], (8, L))
                for t in range(halves):
                    rows = slice(8 * t, 8 * t + 8)
                    lines = [
                        Line(lambda i, g=g: vd[g, c, 8 * t + 3 + i : 8 * t + 11 + i],
                             lambda i, g=g: vs[g, c, 8 * t + 3 + i : 8 * t + 11 + i])
                        for g in range(1 if c in ZERO[1] else 2)
                    ]
                    here = slice(8 * t + 3, 8 * t + 11)
                    double = None if c in ZERO[1] else vt[0, c, here] + vt[1, c, here]
                    f = face(lines[0], lines[1] if len(lines) > 1 else None, double)
                    turned = pltpu.roll(f, 1, 0)
                    lower = jnp.where(sub == 0, before, turned)
                    before = turned
                    patch = pltpu.roll(pd[c, t], lax.rem(L + L - 6 - slot * r, L), 1)
                    rate = jnp.where(edge, patch, acc[c, r, rows])
                    rate = rate + (cth[0, rows] * f - cth[1, rows] * lower)
                    rate = rate + (rp * fr[c, r + 1, rows] - rm * fr[c, r, rows])
                    new[c][t] = w * tile(0, c, r, t) + (1.0 - w) * (tile(stage, c, r, t) + rate)
            for t in range(halves):
                b, d = [new[c][t] for c in range(3)], [new[c][t] for c in range(3, 6)]
                b2 = jnp.maximum(b[0] * b[0] + b[1] * b[1] + b[2] * b[2], 1.0)
                along = (b[0] * d[0] + b[1] * d[1] + b[2] * d[2]) / b2
                d = [y - along * x for x, y in zip(b, d)]
                d2 = d[0] * d[0] + d[1] * d[1] + d[2] * d[2]
                shrink = jnp.sqrt(b2 / jnp.maximum(d2, b2))
                for c in range(3):
                    new[3 + c][t] = d[c] * shrink
                for c in range(6):
                    u[stage + 1, c, base + r, 8 * t : 8 * t + 8] = new[c][t]

            @pl.when(stage < 2)
            def _():
                pack(stage + 1, r, new)

            return carry

        lax.fori_loop(0, nr, final, 0)

        @pl.when(stage < 2)
        def _():
            send_all(stage + 1)

        return carry

    lax.fori_loop(0, 3, stage_body, 0)
    stores = [
        pltpu.make_async_copy(u.at[3, 3 * i : 3 * i + 3, base : base + nr, 0:nt], dst, local.at[i])
        for i, dst in enumerate((mag_out, ele_out))
    ]
    for c in stores:
        c.start()

    def drain(stage, carry):
        @pl.when(has_outer)
        def _():
            radial_out(stage).wait_send()

        @pl.when(has_inner)
        def _():
            radial_in(stage).wait_send()

        for c in theta_copies(stage) + phi_copies(stage):
            c.wait_send()
        return carry

    lax.fori_loop(0, 3, drain, 0)
    for c in stores:
        c.wait()


def solution(mesh):
    n_row, n_theta, n_phi = (mesh.shape[k] for k in ("row", "theta", "phi"))

    def body(magnetic, electric):
        _, nr, nt, lanes = magnetic.shape
        plane = -(-(nt + 2 * G) // 8) * 8
        planes = nr + 2 * G
        halves = nt // 8
        pad8 = lambda n: -(-n // 8) * 8
        f32 = jnp.float32
        vm = lambda *shape: pltpu.VMEM(shape, f32)
        sizes = (n_row, n_theta, n_phi, nr, nt, lanes, plane)
        anywhere = pl.BlockSpec(memory_space=pl.ANY)
        packs = vm(3, 6, halves, 8, lanes)
        joined = vm(3, 2, halves, 8, lanes)
        return pl.pallas_call(
            functools.partial(kernel, sizes),
            out_shape=[jax.ShapeDtypeStruct(magnetic.shape, f32)] * 2,
            in_specs=[anywhere] * 2,
            out_specs=[anywhere] * 2,
            scratch_shapes=[
                vm(4, 6, planes + 2, plane, lanes),
                packs, packs,
                joined, joined, joined, joined,
                vm(3, 2, 6 * G * nr, lanes),
                vm(3, 2, 6 * G * nr, lanes),
                vm(6, nr + 1, nt, lanes),
                vm(6, nr, nt, lanes),
                vm(2, 6, planes, nt, lanes),
                vm(2, 6, nt + 16, lanes),
                vm(2, 6, nt + 16, lanes),
                vm(2, 6, nt + 16, lanes),
                vm(6, pad8(nr), lanes),
                vm(6, halves, 8, lanes),
                vm(pad8(planes), lanes),
                vm(pad8(planes), lanes),
                vm(pad8(nr), lanes),
                vm(pad8(nr), lanes),
                vm(2, nt, lanes),
                pltpu.SemaphoreType.DMA((3, 6)),
                pltpu.SemaphoreType.DMA((3, 6)),
                pltpu.SemaphoreType.DMA((2,)),
            ],
            compiler_params=pltpu.CompilerParams(
                collective_id=0, has_side_effects=True
            ),
        )(magnetic, electric)

    spec = P(None, "row", "theta", "phi")
    return jax.shard_map(body, mesh=mesh, in_specs=(spec, spec), out_specs=(spec, spec), check_vma=False)
```
